32 devices in a mesh: pod: 2 (over x), dp: 4 (over z), sp: 4 (over y, core).
Axes of the slice: x: 2, y: 2, z: 4, core: 2. Of those that a mesh axis runs over, the one named last changes fastest.
Arguments:
- x: bfloat16 [8, 128, 256, 1152], P(('pod', 'dp'), 'sp'), parts along dimension 0
- norm_gain: bfloat16 [2, 2, 1152], replicated
- norm_shift: bfloat16 [2, 2, 1152], replicated
- w_qkv: bfloat16 [2, 3, 1152, 16, 72], replicated
- w_out: bfloat16 [2, 16, 72, 1152], replicated
- w_up: bfloat16 [2, 1152, 4608], replicated
- w_down: bfloat16 [2, 4608, 1152], replicated
Outputs:
- output: bfloat16 [8, 128, 256, 1152], P(('pod', 'dp'), 'sp'), parts along dimension 0
There are 2 independent parts. The reference program is written for one: setup_inputs(seed, part) draws one part's arguments, and reference() takes and returns one part's arrays. A program takes and returns all parts, laid end to end along the dimension named above; an argument that names none is the same for every part.
All inputs are finite; a program needn't handle non-finite values.
Results may differ from the reference program's by a relative error of at most 0.0155992.
Values are sent between devices in bfloat16 or wider.
A program may use at most 1 GiB of HBM per device.

```python
import jax
import jax.numpy as jnp
from jax import lax

NUM_VIDEOS = 4
NUM_FRAMES = 128
NUM_PATCHES = 256
MODEL_WIDTH = 1152
NUM_HEADS = 16

HEAD_DIM = MODEL_WIDTH // NUM_HEADS
FF_WIDTH = 4 * MODEL_WIDTH
LN_EPS = 1e-6
QK_GAIN = 1.5


def layer_norm(tokens, gain, shift):
    tok_f = tokens.astype(jnp.float32)
    mean_val = jnp.mean(tok_f, axis=-1, keepdims=True)
    centered = tok_f - mean_val
    var_val = jnp.mean(centered * centered, axis=-1, keepdims=True)
    normed = centered * lax.rsqrt(var_val + LN_EPS)
    return (normed * gain.astype(jnp.float32) + shift.astype(jnp.float32)).astype(jnp.bfloat16)


def seq_block(tokens, gains, shifts, w_qkv, w_out, w_up, w_down):
    normed = layer_norm(tokens, gains[0], shifts[0])
    proj_qkv = jnp.einsum('ld,kdhe->klhe', normed.astype(jnp.float32), w_qkv.astype(jnp.float32)).astype(jnp.bfloat16)
    scores = jnp.einsum('lhe,mhe->hlm', proj_qkv[0].astype(jnp.float32), proj_qkv[1].astype(jnp.float32)) * (HEAD_DIM ** -0.5)
    attn_probs = jax.nn.softmax(scores, axis=-1).astype(jnp.bfloat16)
    mixed = jnp.einsum('hlm,mhe->lhe', attn_probs.astype(jnp.float32), proj_qkv[2].astype(jnp.float32)).astype(jnp.bfloat16)
    attn_proj = jnp.einsum('lhe,hed->ld', mixed.astype(jnp.float32), w_out.astype(jnp.float32)).astype(jnp.bfloat16)
    hidden = (tokens.astype(jnp.float32) + attn_proj.astype(jnp.float32)).astype(jnp.bfloat16)
    normed_mlp = layer_norm(hidden, gains[1], shifts[1])
    up_proj = jnp.dot(normed_mlp, w_up, preferred_element_type=jnp.float32).astype(jnp.bfloat16)
    activated = jax.nn.gelu(up_proj.astype(jnp.float32), approximate=True).astype(jnp.bfloat16)
    down_proj = jnp.dot(activated, w_down, preferred_element_type=jnp.float32).astype(jnp.bfloat16)
    return (hidden.astype(jnp.float32) + down_proj.astype(jnp.float32)).astype(jnp.bfloat16)


def setup_inputs(seed: int = 0, part: int = 0) -> dict:
    base_key = jax.random.key(seed)
    key_list = jax.random.split(base_key, 7)
    data_key = jax.random.fold_in(key_list[0], part)
    key_frame, key_patch, key_noise = jax.random.split(data_key, 3)
    frame_code = jax.random.normal(key_frame, (NUM_VIDEOS, NUM_FRAMES, 1, MODEL_WIDTH), jnp.float32)
    patch_code = jax.random.normal(key_patch, (NUM_VIDEOS, 1, NUM_PATCHES, MODEL_WIDTH), jnp.float32)
    noise_val = jax.random.normal(key_noise, (NUM_VIDEOS, NUM_FRAMES, NUM_PATCHES, MODEL_WIDTH), jnp.float32)
    x = (frame_code + patch_code + 0.5 * noise_val).astype(jnp.bfloat16)
    norm_gain = (1.0 + 0.4 * jax.random.normal(key_list[1], (2, 2, MODEL_WIDTH), jnp.float32)).astype(jnp.bfloat16)
    norm_shift = (0.4 * jax.random.normal(key_list[2], (2, 2, MODEL_WIDTH), jnp.float32)).astype(jnp.bfloat16)
    qkv_gain = jnp.array([QK_GAIN, QK_GAIN, 1.0], jnp.float32).reshape(1, 3, 1, 1, 1)
    w_qkv = (jax.random.normal(key_list[3], (2, 3, MODEL_WIDTH, NUM_HEADS, HEAD_DIM), jnp.float32) * (MODEL_WIDTH ** -0.5) * qkv_gain).astype(jnp.bfloat16)
    w_out = (jax.random.normal(key_list[4], (2, NUM_HEADS, HEAD_DIM, MODEL_WIDTH), jnp.float32) * (MODEL_WIDTH ** -0.5)).astype(jnp.bfloat16)
    w_up = (jax.random.normal(key_list[5], (2, MODEL_WIDTH, FF_WIDTH), jnp.float32) * (MODEL_WIDTH ** -0.5)).astype(jnp.bfloat16)
    w_down = (jax.random.normal(key_list[6], (2, FF_WIDTH, MODEL_WIDTH), jnp.float32) * (FF_WIDTH ** -0.5)).astype(jnp.bfloat16)
    return {'x': x, 'norm_gain': norm_gain, 'norm_shift': norm_shift, 'w_qkv': w_qkv, 'w_out': w_out, 'w_up': w_up, 'w_down': w_down}


def reference(x, norm_gain, norm_shift, w_qkv, w_out, w_up, w_down):
    num_videos, num_frames, num_patches, model_width = x.shape

    def spatial_fn(frame_tok):
        return seq_block(frame_tok, norm_gain[0], norm_shift[0], w_qkv[0], w_out[0], w_up[0], w_down[0])

    def temporal_fn(tube_tok):
        return seq_block(tube_tok, norm_gain[1], norm_shift[1], w_qkv[1], w_out[1], w_up[1], w_down[1])

    frame_rows = x.reshape(num_videos * num_frames, num_patches, model_width)
    spatial_out = lax.map(spatial_fn, frame_rows).reshape(num_videos, num_frames, num_patches, model_width)
    tube_rows = jnp.transpose(spatial_out, (0, 2, 1, 3)).reshape(num_videos * num_patches, num_frames, model_width)
    temporal_out = lax.map(temporal_fn, tube_rows).reshape(num_videos, num_patches, num_frames, model_width)
    return jnp.transpose(temporal_out, (0, 2, 1, 3))
```

```python
import functools
import math

import jax
import jax.numpy as jnp
from jax import lax
from jax.experimental import pallas as pl
from jax.experimental.pallas import tpu as pltpu
from jax.sharding import PartitionSpec as P

F32, BF = jnp.float32, jnp.bfloat16
D, H, E, FF = 1152, 16, 72, 4608
EP = 80
LN_EPS = 1e-6
NN = (((1,), (0,)), ((), ()))
NT = (((1,), (1,)), ((), ()))
TN = (((0,), (0,)), ((), ()))
CEXP = E ** -0.5 * math.log2(math.e)
SLOTS = 4
QC = 576
UC = 256
DC = 256
LANES = 128
G = 8
MESH = pl.DeviceIdType.MESH


def dg(a, b, dims):
    return lax.dot_general(a, b, dims, preferred_element_type=F32)


def ln(tok, gain, shift):
    mean = jnp.sum(tok, axis=-1, keepdims=True) * (1.0 / D)
    cen = tok - mean
    var = jnp.sum(cen * cen, axis=-1, keepdims=True) * (1.0 / D)
    return cen * lax.rsqrt(var + LN_EPS) * gain + shift


def gelu(u):
    u = u.astype(BF).astype(F32)
    t = jnp.tanh(u * (0.7978845608028654 + 0.035677408136300125 * (u * u)))
    half = 0.5 * u
    return (half + half * t).astype(BF)


def interleave(main, side, weights):
    total, done, k = sum(weights), 0.0, 0
    for thunk, w in zip(main, weights):
        goal = int(done / total * len(side)) + 1
        while k < min(goal, len(side)):
            side[k]()
            k += 1
        thunk()
        done += w
    for thunk in side[k:]:
        thunk()


def peer_of(k):
    me = lax.axis_index("sp")
    yy, cc = me // 2, me % 2
    return 2 * ((yy + k // 2) % 2) + (cc + k % 2) % 2


def entry_barrier():
    bar = pltpu.get_barrier_semaphore()
    for k in (1, 2, 3):
        pl.semaphore_signal(bar, inc=1, device_id={"sp": peer_of(k)}, device_id_type=MESH)
    pl.semaphore_wait(bar, 3)


def col_max(s_ref, k, rows, step=32):
    m = None
    for r in range(0, rows, step):
        t = jnp.max(s_ref[k, r:r + step, :].reshape(step // 8, 8, -1), axis=0)
        m = t if m is None else jnp.maximum(m, t)
    return jnp.max(m, axis=0, keepdims=True)


def softmax_cols(s_ref, k, rows, put, step=32):
    mc = col_max(s_ref, k, rows) * CEXP
    d = None
    for r in range(0, rows, step):
        e = jnp.exp2(s_ref[k, r:r + step, :] * CEXP - mc)
        s_ref[k, r:r + step, :] = e
        t = jnp.sum(e.reshape(step // 8, 8, -1), axis=0)
        d = t if d is None else d + t
    inv = 1.0 / jnp.sum(d, axis=0, keepdims=True)
    for r in range(0, rows, step):
        put(r, step, s_ref[k, r:r + step, :] * inv)


def head_sides(scores, soft, mix, oT_ref):
    pend = {}

    def side(h):
        if h < H:
            scores(h)
        if 0 <= h - 1 < H:
            soft(h - 1)
        if 0 <= h - 2 < H:
            pend[h - 2] = mix(h - 2)[:E]
            if h % 2:
                j = (h - 2) // 2
                pair = jnp.concatenate([pend.pop(2 * j), pend.pop(2 * j + 1)], axis=0)
                oT_ref[2 * E * j:2 * E * (j + 1), :] = pair.astype(BF)

    return [functools.partial(side, h) for h in range(H + 2)]


def load_weights(pairs, sem):
    return [pltpu.make_async_copy(src, dst, sem.at[i]) for i, (src, dst) in enumerate(pairs)]


def spatial_kernel(FR, NPQ, x_ref, xn_ref, gain_ref, shift_ref, wq_hbm, wo_hbm, wu_hbm, wd_hbm, xs_hbm, rcv_hbm,
                   wq, wo, wu, wd, n1, hh, qkv, s_ref, p_ref, oT, n2, g_ref, obuf, wsem, lsem, ssem, rsem):
    i = pl.program_id(0)
    NP = 4 * NPQ
    me = lax.axis_index("sp")
    loads = load_weights([(wq_hbm.at[0], wq), (wo_hbm.at[0], wo), (wu_hbm.at[0], wu), (wd_hbm.at[0], wd)], wsem)
    g1, b1 = gain_ref[0, 0:1, :].astype(F32), shift_ref[0, 0:1, :].astype(F32)
    g2, b2 = gain_ref[0, 1:2, :].astype(F32), shift_ref[0, 1:2, :].astype(F32)

    def copies(slot, f):
        local = [
            pltpu.make_async_copy(obuf.at[slot], xs_hbm.at[:, f], lsem.at[slot, 0]),
            pltpu.make_async_copy(obuf.at[slot, me], rcv_hbm.at[me, f], lsem.at[slot, 1]),
        ]
        remote = [
            pltpu.make_async_remote_copy(
                src_ref=obuf.at[slot, peer_of(k)], dst_ref=rcv_hbm.at[me, f],
                send_sem=ssem.at[slot, k - 1], recv_sem=rsem.at[k - 1],
                device_id={"sp": peer_of(k)}, device_id_type=MESH)
            for k in (2, 3, 1)
        ]
        return local, remote

    def wait_slot(slot, f):
        local, remote = copies(slot, f)
        for c in local:
            c.wait()
        for c in remote:
            c.wait_send()

    def step(do_a, do_b):
        f = i - 1
        slot = lax.rem(f + 2, 2)
        if do_b:
            pl.when(f >= 2)(lambda: wait_slot(slot, f - 2))

        def ln1(src):
            def part(r):
                n1[r:r + 64, :] = ln(src[0, r:r + 64, :].astype(F32), g1, b1).astype(BF)
            return [functools.partial(part, r) for r in range(0, NP, 64)]

        def ln2_part(r):
            n2[r:r + 64, :] = ln(hh[r:r + 64, :].astype(F32), g2, b2).astype(BF)

        def proj(t, c):
            r = dg(wq[t * D + c * QC:t * D + (c + 1) * QC, :], n1[...], NT)
            z = jnp.zeros((EP - E, NP), F32)
            for h in range(QC // E):
                qkv[t, c * (QC // E) + h] = jnp.concatenate([r[h * E:(h + 1) * E], z], axis=0).astype(BF)

        def up(c):
            u = dg(n2[...], wu[:, c * UC:(c + 1) * UC], NN)
            g_ref[:, c * UC:(c + 1) * UC] = gelu(u)

        def down(c):
            e = min(c + DC, D)
            m = dg(g_ref[...], wd[:, c:e], NN).astype(BF).astype(F32)
            for q in range(4):
                old = obuf[slot, q, :, c:e].astype(F32)
                obuf[slot, q, :, c:e] = (old + m[q * NPQ:(q + 1) * NPQ]).astype(BF)

        def outp():
            a = dg(oT[...], wo[...], TN).astype(BF)
            hh[...] = (x_ref[0].astype(F32) + a.astype(F32)).astype(BF)

        def scores(h):
            s_ref[h % SLOTS] = dg(qkv[1, h], qkv[0, h], TN)

        def soft(h):
            k = h % SLOTS

            def put(r, n, v):
                p_ref[k, r:r + n, :] = v.astype(BF)
            softmax_cols(s_ref, k, NP, put)

        def mix(h):
            return dg(qkv[2, h], p_ref[h % SLOTS], NN)

        projs = [functools.partial(proj, t, c) for c in range(D // QC) for t in range(3)]
        ups = [functools.partial(up, c) for c in range(FF // UC)]
        downs = [functools.partial(down, c) for c in range(0, D, DC)]
        heads = head_sides(scores, soft, mix, oT)
        ln2s = [functools.partial(ln2_part, r) for r in range(0, NP, 64)]

        if do_b:
            for q in range(4):
                obuf[slot, q] = hh[q * NPQ:(q + 1) * NPQ, :]
        if do_a and do_b:
            interleave(projs, ln2s, [1.0] * len(projs))
            interleave(ups + downs[:-1], heads, [5.0] * len(ups) + [18.0] * (len(downs) - 1))
            interleave([outp, downs[-1]], ln1(xn_ref), [0.0, 1.0])
        elif do_a:
            for th in ln1(x_ref) + projs + heads + [outp] + ln1(xn_ref):
                th()
        else:
            for th in ln2s + ups + downs:
                th()

        if do_b:
            local, remote = copies(slot, f)
            for c in remote + local:
                c.start()

    @pl.when(i == 0)
    def _():
        for c in loads:
            c.start()
        entry_barrier()
        for c in loads[:2]:
            c.wait()
        step(True, False)

    @pl.when(i == 1)
    def _():
        for c in loads[2:]:
            c.wait()

    pl.when((i > 0) & (i < FR))(lambda: step(True, True))

    @pl.when(i == FR)
    def _():
        step(False, True)
        for f in (FR - 2, FR - 1):
            wait_slot(f % 2, f)
        for k in (1, 2, 3):
            src = peer_of(k)
            pltpu.make_async_copy(rcv_hbm.at[src], rcv_hbm.at[src], rsem.at[k - 1]).wait()


def spatial(x, gain, shift, wq, wo, wu, wd):
    FR, NP, _ = x.shape
    NPQ = NP // 4
    any_spec = pl.BlockSpec(memory_space=pl.ANY)
    vm = pltpu.VMEM
    part = jax.ShapeDtypeStruct((4, FR, NPQ, D), BF)
    flops = 2 * FR * NP * (4 * D * D + 2 * D * FF) + 4 * FR * NP * NP * D
    return pl.pallas_call(
        functools.partial(spatial_kernel, FR, NPQ),
        grid=(FR + 1,),
        in_specs=[
            pl.BlockSpec((1, NP, D), lambda i: (jnp.minimum(i, FR - 1), 0, 0)),
            pl.BlockSpec((1, NP, D), lambda i: (jnp.minimum(i + 1, FR - 1), 0, 0)),
            pl.BlockSpec((2, 2, D), lambda i: (0, 0, 0)),
            pl.BlockSpec((2, 2, D), lambda i: (0, 0, 0)),
            any_spec, any_spec, any_spec, any_spec,
        ],
        out_specs=[any_spec, any_spec],
        out_shape=[part, part],
        scratch_shapes=[
            vm((3 * D, D), BF), vm((D, D), BF), vm((D, FF), BF), vm((FF, D), BF),
            vm((NP, D), BF), vm((NP, D), BF), vm((3, H, EP, NP), BF),
            vm((SLOTS, NP, NP), F32), vm((SLOTS, NP, NP), BF), vm((D, NP), BF),
            vm((NP, D), BF), vm((NP, FF), BF), vm((2, 4, NPQ, D), BF),
            pltpu.SemaphoreType.DMA((4,)), pltpu.SemaphoreType.DMA((2, 2)),
            pltpu.SemaphoreType.DMA((2, 3)), pltpu.SemaphoreType.DMA((3,)),
        ],
        compiler_params=pltpu.CompilerParams(
            collective_id=0, has_side_effects=True, vmem_limit_bytes=60 * 1024 * 1024,
            dimension_semantics=("arbitrary",)),
        cost_estimate=pl.CostEstimate(flops=flops, bytes_accessed=4 * x.size * 2, transcendentals=0),
        name="spatial",
    )(x, x, gain, shift, wq, wo, wu, wd)


def temporal_kernel(FR, NPQ, rcv_hbm, xs_hbm, gain_ref, shift_ref, wq_hbm, wo_hbm, wu_hbm, wd_hbm,
                    y_hbm, o_hbm, orcv_hbm,
                    wq, wo, wu, wsem, xsem, lsem, ssem, rsem, bsem, ysem):
    KF = 4 * FR
    NG = NPQ // G
    T = 2 * KF
    B = FR * G
    NCOL = D // LANES
    S = KF + 8
    PJ = G // 2
    assert PJ == 4
    NT_ = NG * PJ
    me = lax.axis_index("sp")
    loads = load_weights([(wq_hbm.at[1], wq), (wo_hbm.at[1], wo), (wu_hbm.at[1], wu)], wsem)
    for c in loads:
        c.start()
    g1, b1 = gain_ref[1, 0:1, :].astype(F32), shift_ref[1, 0:1, :].astype(F32)
    g2, b2 = gain_ref[1, 1:2, :].astype(F32), shift_ref[1, 1:2, :].astype(F32)
    entry_barrier()

    def send(g, k):
        at = pl.ds(pl.multiple_of(g * G, G), G)
        return pltpu.make_async_remote_copy(
            src_ref=o_hbm.at[peer_of(k), :, at], dst_ref=orcv_hbm.at[me, :, at],
            send_sem=ssem.at[k - 1, g], recv_sem=rsem.at[k - 1, g],
            device_id={"sp": peer_of(k)}, device_id_type=MESH)

    def phase1(nscr, oscr, xblk, nb, qb, kb, vb, s_ref, p_ref, oT, oblk):
        def x_load(g, slot):
            at = pl.ds(pl.multiple_of(g * G, G), G)
            return pltpu.make_async_copy(rcv_hbm.at[:, :, at], xblk.at[slot], xsem.at[slot])

        def o_store(g):
            at = pl.ds(pl.multiple_of(g * G, G), G)
            return [
                pltpu.make_async_copy(oblk, o_hbm.at[:, :, at], lsem.at[0]),
                pltpu.make_async_copy(oblk.at[me], orcv_hbm.at[me, :, at], lsem.at[1]),
            ]

        def ln_part(slot, par, a, r):
            tok = xblk[slot, a, 8 * r:8 * r + 8].astype(F32).reshape(8 * G, D)
            n = ln(tok, g1, b1)
            for fi in range(8):
                f = a * FR + 8 * r + fi
                for c in range(NCOL):
                    nscr[par, c, pl.ds(f, G, stride=S), :] = n[fi * G:(fi + 1) * G, c * LANES:(c + 1) * LANES]

        def take_pair(par, j):
            for e in range(2):
                at = pl.ds(pl.multiple_of((2 * j + e) * S, 8), KF)
                for c in range(NCOL):
                    nb[e * KF:(e + 1) * KF, c * LANES:(c + 1) * LANES] = nscr[par, c, at, :].astype(BF)

        def proj(par, t, c):
            r = dg(wq[t * D + c * QC:t * D + (c + 1) * QC, :], nb[...], NT)
            z = jnp.zeros((EP - E, T), F32)
            for hi in range(QC // E):
                h = c * (QC // E) + hi
                v = jnp.concatenate([r[hi * E:(hi + 1) * E], z], axis=0).astype(BF)
                if t == 2:
                    vb[par, h] = v
                else:
                    for e in range(2):
                        w = v[:, e * KF:(e + 1) * KF]
                        if t == 0:
                            qb[par, h, e * EP:(e + 1) * EP, e * KF:(e + 1) * KF] = w
                        else:
                            kb[par, h, e * EP:(e + 1) * EP, :] = w

        def heads(par):
            def scores(h):
                s_ref[h % SLOTS] = dg(kb[par, h], qb[par, h], TN)

            def soft(h):
                k = h % SLOTS

                def put(r, n, v):
                    v = v.astype(BF)
                    p_ref[k, r:r + n, 0:KF] = v[:, 0:KF]
                    p_ref[k, KF + r:KF + r + n, KF:T] = v[:, KF:T]
                softmax_cols(s_ref, k, KF, put)

            def mix(h):
                return dg(vb[par, h], p_ref[h % SLOTS], NN)

            return head_sides(scores, soft, mix, oT)

        def put_pair(par, j):
            for e in range(2):
                at = pl.ds(pl.multiple_of((2 * j + e) * S, 8), KF)
                for c in range(NCOL):
                    v = oT[c * LANES:(c + 1) * LANES, e * KF:(e + 1) * KF]
                    oscr[par, c, at, :] = jnp.transpose(v).astype(F32)

        def gather_part(par, a, r):
            for fi in range(8):
                f = a * FR + 8 * r + fi
                row = [oscr[par, c, pl.ds(f, G, stride=S), :] for c in range(NCOL)]
                oblk[a, 8 * r + fi] = jnp.concatenate(row, axis=1).astype(BF)

        x_load(0, 0).start()
        x_load(1, 1).start()
        qb[...] = jnp.zeros_like(qb)
        p_ref[...] = jnp.zeros_like(p_ref)
        kb[...] = jnp.zeros_like(kb)
        vb[...] = jnp.zeros_like(vb)
        x_load(0, 0).wait()

        def first(a, _):
            for r in range(FR // 8):
                ln_part(0, 0, a, r)
            return 0
        lax.fori_loop(0, 4, first, 0)
        loads[0].wait()

        def body(t, _):
            g, j = t // PJ, t % PJ
            ga, a = (t + 3) // PJ - 2, (t + 3) % PJ

            @pl.when(j == 0)
            def _():
                @pl.when(g + 1 < NG)
                def _():
                    x_load(g + 1, (g + 1) % 2).wait()

                @pl.when(g + 2 < NG)
                def _():
                    x_load(g + 2, g % 2).start()

            @pl.when((a == 0) & (ga >= 1))
            def _():
                for c in o_store(ga - 1):
                    c.wait()
                for k in (2, 3, 1):
                    send(ga - 1, k).start()

            par, gp = t % 2, g % 2
            hp, hg, hj = (t + 1) % 2, ((t + 7) // PJ) % 2, (t + 7) % PJ
            take_pair(gp, j)
            main = [functools.partial(proj, par, tt, c) for c in range(D // QC) for tt in range(3)]
            side = heads(hp)
            lns = [functools.partial(ln_part, (g + 1) % 2, (g + 1) % 2, j, r) for r in range(FR // 8)]
            gas = [functools.partial(gather_part, (ga + 2) % 2, a, r) for r in range(FR // 8)]
            extra = [th for pair in zip(lns, gas) for th in pair]
            merged, k = [], 0
            for n, th in enumerate(side):
                merged.append(th)
                if n % 2 == 1 and k < len(extra):
                    merged.append(extra[k])
                    k += 1
            merged += extra[k:]
            interleave(main, merged, [1.0] * len(main))
            put_pair(hg, hj)

            @pl.when((a == PJ - 1) & (ga >= 0))
            def _():
                for c in o_store(ga):
                    c.start()
            return 0
        lax.fori_loop(0, NT_, body, 0)

        for th in heads((NT_ - 1) % 2):
            th()
        put_pair((NG - 1) % 2, PJ - 1)

        def finish(g):
            for c in o_store(g):
                c.start()
            for c in o_store(g):
                c.wait()
            for k in (2, 3, 1):
                send(g, k).start()
        for r in range(FR // 8):
            gather_part((NG - 2) % 2, 3, r)
        finish(NG - 2)

        def last(a, _):
            for r in range(FR // 8):
                gather_part((NG - 1) % 2, a, r)
            return 0
        lax.fori_loop(0, 4, last, 0)
        finish(NG - 1)

    NB = 4 * NG

    def phase2(wd, ob, xb, yb, of, hh, n2, g_ref):
        wd_load = pltpu.make_async_copy(wd_hbm.at[1], wd, wsem.at[3])
        wd_load.start()

        def block(b):
            return peer_of(b // NG), b % NG

        def fetch(b, slot):
            owner, g = block(b)
            at = pl.ds(pl.multiple_of(g * G, G), G)
            return [
                pltpu.make_async_copy(orcv_hbm.at[owner, :, at], ob.at[slot], bsem.at[slot, 0]),
                pltpu.make_async_copy(xs_hbm.at[owner, :, at], xb.at[slot], bsem.at[slot, 1]),
            ]

        def arrive(b):
            owner, g = block(b)
            at = pl.ds(pl.multiple_of(g * G, G), G)
            here = orcv_hbm.at[owner, :, at]
            return pltpu.make_async_copy(here, here, rsem.at[b // NG - 1, g])

        def y_store(b, slot):
            owner, g = block(b)
            at = pl.ds(pl.multiple_of(owner * NPQ + g * G, G), G)
            return pltpu.make_async_copy(yb.at[slot], y_hbm.at[:, at], ysem.at[slot])

        def ln2_part(r):
            n2[r:r + 64, :] = ln(hh[r:r + 64, :].astype(F32), g2, b2).astype(BF)
        ln2s = [functools.partial(ln2_part, r) for r in range(0, B, 64)]

        def take(slot, c):
            e = min(c + DC, D)
            of[:, c:e] = ob[slot, :, :, c:e].astype(F32).reshape(B, e - c).astype(BF)

        def outp(slot, c):
            e = min(c + DC, D)
            x = xb[slot, :, :, c:e].astype(F32).reshape(B, e - c)
            a = dg(of[...], wo[:, c:e], NN).astype(BF)
            hh[:, c:e] = (x + a.astype(F32)).astype(BF)

        def up(c):
            u = dg(n2[...], wu[:, c * UC:(c + 1) * UC], NN)
            g_ref[:, c * UC:(c + 1) * UC] = gelu(u)

        def down(slot, c):
            e = min(c + DC, D)
            m = dg(g_ref[...], wd[:, c:e], NN).astype(BF).astype(F32)
            old = yb[slot, :, :, c:e].astype(F32)
            yb[slot, :, :, c:e] = (old + m.reshape(FR, G, e - c)).astype(BF)

        def step(b, do_a, do_b):
            slot, old = b % 2, (b + 1) % 2
            ups = [functools.partial(up, c) for c in range(FF // UC)]
            outs = [functools.partial(outp, slot, c) for c in range(0, D, DC)]
            downs = [functools.partial(down, old, c) for c in range(0, D, DC)]
            takes = [functools.partial(take, slot, c) for c in range(0, D, DC)]
            if do_b:
                yb[old] = hh[...].astype(F32).reshape(FR, G, D).astype(BF)
            if do_a and do_b:
                interleave(ups, takes, [1.0] * len(ups))
                for th in outs:
                    th()
                interleave(downs, ln2s, [1.0] * len(downs))
            elif do_a:
                for th in takes + outs + ln2s:
                    th()
            else:
                for th in ups + downs:
                    th()

        for c in fetch(0, 0):
            c.start()
        for c in fetch(0, 0):
            c.wait()
        for c in fetch(1, 1):
            c.start()
        loads[1].wait()
        step(0, True, False)
        loads[2].wait()
        wd_load.wait()

        def body(b, _):
            slot = b % 2
            for c in fetch(b, slot):
                c.wait()

            @pl.when(b + 1 < NB)
            def _():
                pl.when(b + 1 >= NG)(lambda: arrive(b + 1).wait())
                for c in fetch(b + 1, (b + 1) % 2):
                    c.start()
            pl.when(b >= 3)(lambda: y_store(b - 3, (b + 1) % 2).wait())
            step(b, True, True)
            y_store(b - 1, (b + 1) % 2).start()
            return 0
        lax.fori_loop(1, NB, body, 0)

        y_store(NB - 3, (NB - 3) % 2).wait()
        step(NB, False, True)
        y_store(NB - 1, (NB - 1) % 2).start()
        for b in (NB - 2, NB - 1):
            y_store(b, b % 2).wait()

    vm = pltpu.VMEM
    pl.run_scoped(
        phase1,
        vm((2, NCOL, G * S, LANES), F32), vm((2, NCOL, G * S, LANES), F32), vm((2, 4, FR, G, D), BF), vm((T, D), BF),
        vm((2, H, 2 * EP, T), BF), vm((2, H, 2 * EP, KF), BF), vm((2, H, EP, T), BF),
        vm((SLOTS, KF, T), F32), vm((SLOTS, T, T), BF), vm((D, T), BF), vm((4, FR, G, D), BF))
    pl.run_scoped(
        phase2,
        vm((FF, D), BF), vm((2, FR, G, D), BF), vm((2, FR, G, D), BF), vm((2, FR, G, D), BF),
        vm((B, D), BF), vm((B, D), BF), vm((B, D), BF), vm((B, FF), BF))

    def drain(g, _):
        for k in (1, 2, 3):
            send(g, k).wait_send()
        return 0
    lax.fori_loop(0, NG, drain, 0)


def temporal(rcv, xs, gain, shift, wq, wo, wu, wd):
    _, FR, NPQ, _ = rcv.shape
    NG = NPQ // G
    any_spec = pl.BlockSpec(memory_space=pl.ANY)
    full = pl.BlockSpec(memory_space=pltpu.VMEM)
    vm = pltpu.VMEM
    part = jax.ShapeDtypeStruct((4, FR, NPQ, D), BF)
    toks = 4 * FR * NPQ
    flops = 2 * toks * (4 * D * D + 2 * D * FF) + 4 * toks * 4 * FR * D
    y, _, _ = pl.pallas_call(
        functools.partial(temporal_kernel, FR, NPQ),
        in_specs=[any_spec, any_spec, full, full, any_spec, any_spec, any_spec, any_spec],
        out_specs=[any_spec, any_spec, any_spec],
        out_shape=[jax.ShapeDtypeStruct((FR, 4 * NPQ, D), BF), part, part],
        scratch_shapes=[
            vm((3 * D, D), BF), vm((D, D), BF), vm((D, FF), BF),
            pltpu.SemaphoreType.DMA((4,)), pltpu.SemaphoreType.DMA((2,)), pltpu.SemaphoreType.DMA((2,)),
            pltpu.SemaphoreType.DMA((3, NG)), pltpu.SemaphoreType.DMA((3, NG)),
            pltpu.SemaphoreType.DMA((2, 2)), pltpu.SemaphoreType.DMA((2,)),
        ],
        compiler_params=pltpu.CompilerParams(
            collective_id=1, has_side_effects=True, vmem_limit_bytes=62 * 1024 * 1024),
        cost_estimate=pl.CostEstimate(flops=flops, bytes_accessed=6 * rcv.size * 2, transcendentals=0),
        name="temporal",
    )(rcv, xs, gain, shift, wq, wo, wu, wd)
    return y


def solution(mesh):
    tok_spec = P(("pod", "dp"), "sp", None, None)

    def local_step(x, gain, shift, w_qkv, w_out, w_up, w_down):
        wq = jnp.transpose(w_qkv, (0, 1, 3, 4, 2)).reshape(2, 3 * D, D)
        wo = w_out.reshape(2, D, D)
        xs, rcv = spatial(x[0], gain, shift, wq, wo, w_up, w_down)
        return temporal(rcv, xs, gain, shift, wq, wo, w_up, w_down)[None]

    return jax.shard_map(local_step, mesh=mesh, in_specs=(tok_spec, P(), P(), P(), P(), P(), P()), out_specs=tok_spec, check_vma=False)
```
